16 devices in a mesh: rep: 4 (over y, z, core), dp: 4 (over x).
Axes of the slice: x: 4, y: 2, z: 1, core: 2. Of those that a mesh axis runs over, the one named last changes fastest.
The devices are a block of a 4x4x8 slice.
Arguments:
- a: bfloat16 [16, 4, 4096, 640], P(('rep', 'dp')), parts along dimension 0
- g: bfloat16 [16, 4, 4096, 2048], P(('rep', 'dp')), parts along dimension 0
Outputs:
- output: bfloat16 [16, 640, 2048], P('rep'), parts along dimension 0
There are 4 independent parts. The reference program is written for one: setup_inputs(seed, part) draws one part's arguments, and reference() takes and returns one part's arrays. A program takes and returns all parts, laid end to end along the dimension named above; each array names one.
All inputs are finite; a program needn't handle non-finite values.
Results may differ from the reference program's by a relative error of at most 0.012.
Values are sent between devices in bfloat16 or wider.
A program may use at most 768 MiB of HBM per device.

```python
import jax
import jax.numpy as jnp
from jax import lax

DEVICES = 4
MATRICES = 4
TOKENS = 4096
D = 640
FF = 2048


def setup_inputs(seed: int = 0, part: int = 0) -> dict:
    ka, kg, ks = (jax.random.fold_in(k, part) for k in jax.random.split(jax.random.key(seed), 3))
    size = 2.0 ** jax.random.uniform(ks, (DEVICES, MATRICES, 1, 1), jnp.float32, -1.0, 1.0)
    a = jax.random.normal(ka, (DEVICES, MATRICES, TOKENS, D), jnp.float32)
    g = size * jax.random.normal(kg, (DEVICES, MATRICES, TOKENS, FF), jnp.float32) * (DEVICES * TOKENS) ** -0.5
    return {"a": a.astype(jnp.bfloat16), "g": g.astype(jnp.bfloat16)}


def reference(a, g):
    def take(so_far, one):
        return so_far + jnp.einsum("ntd,ntf->ndf", *one, preferred_element_type=jnp.float32), None

    return lax.scan(take, jnp.zeros((MATRICES, D, FF), jnp.float32), (a, g))[0].astype(jnp.bfloat16)
```

```python
import jax
import jax.numpy as jnp
from jax import lax
from jax.sharding import PartitionSpec as P


def solution(mesh):
    def local(a, g):
        sums = []
        for n in range(a.shape[1]):
            term = lax.dot_general(
                a[0, n], g[0, n], (((0,), (0,)), ((), ())), preferred_element_type=jnp.float32
            )
            sums.append(lax.psum(term.astype(jnp.bfloat16), "dp"))
        return jnp.stack(sums)

    return jax.shard_map(
        local,
        mesh=mesh,
        in_specs=(P(("rep", "dp")), P(("rep", "dp"))),
        out_specs=P("rep"),
        check_vma=False,
    )
```

```python
import functools

import jax
import jax.numpy as jnp
from jax import lax
from jax.experimental import pallas as pl
from jax.experimental.pallas import tpu as pltpu
from jax.sharding import PartitionSpec as P

MESH = pl.DeviceIdType.MESH
RIGHT, LEFT = 0, 1
FAR, RAW, SUM, FIRST, SECOND, ON = range(6)
G_SLOTS = 3


def kernel(n, a, g, out, abuf, gbuf, term, snd, rcv, fin, a_sem, g_sem, send_sem, recv_sem, out_sem):
    matrices, tokens, rows = a.shape[1:]
    half = g.shape[3] // n // 2
    units = matrices * n
    me = lax.axis_index("dp")
    to = [lax.rem(me + 1, n), lax.rem(me + n - 1, n)]

    def columns(owner, h):
        return pl.ds(pl.multiple_of(owner * (2 * half) + h * half, half), half)

    def load_a(m):
        return pltpu.make_async_copy(a.at[0, m], abuf.at[lax.rem(m, 2)], a_sem.at[lax.rem(m, 2)])

    def load_g(u):
        m, k = u // n, lax.rem(u, n)
        offset = jnp.where(k == 0, 2, jnp.where(k == 1, 1, jnp.where(k == 2, n - 1, 0)))
        owner = lax.rem(me + offset, n)
        slot = lax.rem(u, G_SLOTS)
        src = g.at[0, m, :, pl.ds(pl.multiple_of(owner * (2 * half), 2 * half), 2 * half)]
        return pltpu.make_async_copy(src, gbuf.at[slot], g_sem.at[slot])

    def copy(m, kind, way):
        if kind <= SUM:
            src, dst = snd.at[m, kind, way], rcv.at[m, kind, way]
        elif kind == ON:
            where = out.at[m, :, columns(to[1 - way], way)]
            src, dst = where, where
        else:
            h = way if kind == FIRST else 1 - way
            src, dst = fin.at[m, h], out.at[m, :, columns(me, h)]
        return pltpu.make_async_remote_copy(
            src_ref=src,
            dst_ref=dst,
            send_sem=send_sem.at[m, kind, way],
            recv_sem=recv_sem.at[m, kind, way],
            device_id={"dp": to[way]},
            device_id_type=MESH,
        )

    def keep(m, h):
        return pltpu.make_async_copy(fin.at[m, h], out.at[m, :, columns(me, h)], out_sem.at[m, h])

    def send(m, kind, way, value):
        snd[m, kind, way] = value.astype(snd.dtype)
        copy(m, kind, way).start()

    def add_far(m):
        for way in (RIGHT, LEFT):
            copy(m, FAR, way).wait_recv()
            own = term[lax.rem(m, 2), 1 + way, 1 - way]
            send(m, SUM, way, own + rcv[m, FAR, way].astype(jnp.float32))

    def finish(m):
        for h in (0, 1):
            copy(m, RAW, h).wait_recv()
            copy(m, SUM, 1 - h).wait_recv()
            total = term[lax.rem(m, 2), 3, h] + rcv[m, RAW, h].astype(jnp.float32)
            total = total + rcv[m, SUM, 1 - h].astype(jnp.float32)
            fin[m, h] = total.astype(fin.dtype)
        copy(m, FIRST, RIGHT).start()
        copy(m, FIRST, LEFT).start()
        copy(m, SECOND, RIGHT).start()
        copy(m, SECOND, LEFT).start()
        for h in (0, 1):
            keep(m, h).start()

    def pass_on(m):
        for way in (RIGHT, LEFT):
            copy(m, FIRST, way).wait_recv()
            copy(m, ON, way).start()

    load_a(0).start()
    load_g(0).start()
    load_g(1).start()

    barrier = pltpu.get_barrier_semaphore()
    for way in (RIGHT, LEFT):
        pl.semaphore_signal(barrier, inc=1, device_id={"dp": to[way]}, device_id_type=MESH)
    pl.semaphore_wait(barrier, 2)

    @pl.loop(0, units)
    def unit(u):
        m, k = u // n, lax.rem(u, n)

        @pl.when(u + 2 < units)
        def _():
            load_g(u + 2).start()

        @pl.when(k == 0)
        def _():
            load_a(m).wait()

            @pl.when(m + 1 < matrices)
            def _():
                load_a(m + 1).start()

        load_g(u).wait()
        slot, side = lax.rem(u, G_SLOTS), lax.rem(m, 2)

        @pl.loop(0, 2)
        def _(h):
            at = pl.ds(pl.multiple_of(h * half, half), half)
            term[side, k, h] = lax.dot_general(
                abuf[side], gbuf[slot, :, at], (((0,), (0,)), ((), ())), preferred_element_type=jnp.float32
            )

        @pl.when(k == 0)
        def _():
            send(m, FAR, RIGHT, term[side, 0, 1])
            send(m, FAR, LEFT, term[side, 0, 0])

        @pl.when(k == 1)
        def _():
            send(m, RAW, RIGHT, term[side, 1, 0])

        @pl.when(k == 2)
        def _():
            send(m, RAW, LEFT, term[side, 2, 1])

        @pl.when(k == 3)
        def _():
            add_far(m)

            @pl.when(m >= 1)
            def _():
                finish(m - 1)

            @pl.when(m >= 2)
            def _():
                pass_on(m - 2)

    finish(matrices - 1)
    pass_on(matrices - 2)
    pass_on(matrices - 1)

    @pl.loop(0, matrices)
    def _(m):
        for h in (0, 1):
            keep(m, h).wait()
        for way in (RIGHT, LEFT):
            for kind in (SECOND, ON):
                copy(m, kind, way).wait_recv()
            for kind in range(6):
                copy(m, kind, way).wait_send()


def solution(mesh):
    n = mesh.shape["dp"]

    def local(a, g):
        matrices, tokens, rows = a.shape[1:]
        wide = g.shape[3]
        half = wide // n // 2
        bf16, f32 = jnp.bfloat16, jnp.float32
        return pl.pallas_call(
            functools.partial(kernel, n),
            out_shape=jax.ShapeDtypeStruct((matrices, rows, wide), bf16),
            in_specs=[pl.BlockSpec(memory_space=pl.ANY)] * 2,
            out_specs=pl.BlockSpec(memory_space=pl.ANY),
            scratch_shapes=[
                pltpu.VMEM((2, tokens, rows), bf16),
                pltpu.VMEM((G_SLOTS, tokens, 2 * half), bf16),
                pltpu.VMEM((2, n, 2, rows, half), f32),
                pltpu.VMEM((matrices, 3, 2, rows, half), bf16),
                pltpu.VMEM((matrices, 3, 2, rows, half), bf16),
                pltpu.VMEM((matrices, 2, rows, half), bf16),
                pltpu.SemaphoreType.DMA((2,)),
                pltpu.SemaphoreType.DMA((G_SLOTS,)),
                pltpu.SemaphoreType.DMA((matrices, 6, 2)),
                pltpu.SemaphoreType.DMA((matrices, 6, 2)),
                pltpu.SemaphoreType.DMA((matrices, 2)),
            ],
            compiler_params=pltpu.CompilerParams(
                collective_id=0, has_side_effects=True, vmem_limit_bytes=67043328
            ),
        )(a, g)

    return jax.shard_map(
        local,
        mesh=mesh,
        in_specs=(P(("rep", "dp")), P(("rep", "dp"))),
        out_specs=P("rep"),
        check_vma=False,
    )
```

```python
import functools

import jax
import jax.numpy as jnp
from jax import lax
from jax.experimental import pallas as pl
from jax.experimental.pallas import tpu as pltpu
from jax.sharding import PartitionSpec as P

MESH = pl.DeviceIdType.MESH
RIGHT, LEFT = 0, 1
FAR0, FAR1, RAW, SUM, FIRST, SECOND, ON = range(7)
KINDS = 7
G_SLOTS = 4
CUT = 256
VMEM_LIMIT = 53000000


def kernel(n, a, g, out, abuf, gbuf, term, snd, rcv, a_sem, g_sem, send_sem, recv_sem):
    matrices, tokens, rows = a.shape[1:]
    half = g.shape[3] // n // 2
    per = 2 * n
    units = matrices * per
    f32 = jnp.float32
    me = lax.axis_index("dp")
    to = [lax.rem(me + 1, n), lax.rem(me + n - 1, n)]

    def columns(owner, h):
        return pl.ds(pl.multiple_of(owner * (2 * half) + h * half, half), half)

    def load_a(m):
        return pltpu.make_async_copy(a.at[0, m], abuf.at[lax.rem(m, 2)], a_sem.at[lax.rem(m, 2)])

    def load_a_part(part):
        at = pl.ds(0, CUT) if part == 0 else pl.ds(CUT, rows - CUT)
        return pltpu.make_async_copy(a.at[0, 0, :, at], abuf.at[0, :, at], a_sem.at[2 * part])

    def pick(j, values):
        out = values[-1]
        for i, value in reversed(list(enumerate(values[:-1]))):
            out = jnp.where(j == i, value, out)
        return out

    order = [(2, 1), (2, 0), (1, 0), (n - 1, 1), (1, 1), (n - 1, 0), (0, 0), (0, 1)]

    def load_g(u):
        m, j = u // per, lax.rem(u, per)
        owner = lax.rem(me + pick(j, [o for o, _ in order]), n)
        slot = lax.rem(u, G_SLOTS)
        src = g.at[0, m, :, columns(owner, pick(j, [h for _, h in order]))]
        return pltpu.make_async_copy(src, gbuf.at[slot], g_sem.at[slot])

    def copy(m, kind, way):
        if kind in (FAR0, FAR1):
            at = pl.ds(0, CUT) if kind == FAR0 else pl.ds(CUT, rows - CUT)
            src, dst = snd.at[m, 0, way, at], rcv.at[m, 0, way, at]
        elif kind in (RAW, SUM):
            src, dst = snd.at[m, kind - 1, way], rcv.at[m, kind - 1, way]
        else:
            owner = to[1 - way] if kind == ON else me
            h = 1 - way if kind == SECOND else way
            src = dst = out.at[m, :, columns(owner, h)]
        return pltpu.make_async_remote_copy(
            src_ref=src,
            dst_ref=dst,
            send_sem=send_sem.at[m, kind, way],
            recv_sem=recv_sem.at[m, kind, way],
            device_id={"dp": to[way]},
            device_id_type=MESH,
        )

    def add_far(m):
        for way in (RIGHT, LEFT):
            copy(m, FAR0, way).wait_recv()
            copy(m, FAR1, way).wait_recv()
            total = term[1 + way] + rcv[m, 0, way].astype(f32)
            snd[m, 2, way] = total.astype(snd.dtype)
            copy(m, SUM, way).start()

    def finish(m):
        for h in (0, 1):
            copy(m, RAW, h).wait_recv()
            copy(m, SUM, 1 - h).wait_recv()
            total = term[3 + 2 * lax.rem(m, 2) + h] + rcv[m, 1, h].astype(f32)
            total = total + rcv[m, 2, 1 - h].astype(f32)
            out[m, :, columns(me, h)] = total.astype(out.dtype)
            copy(m, FIRST, h).start()
        copy(m, SECOND, RIGHT).start()
        copy(m, SECOND, LEFT).start()

    def pass_on(m):
        for way in (RIGHT, LEFT):
            copy(m, FIRST, way).wait_recv()
            copy(m, ON, way).start()

    def dot(x, y):
        return lax.dot_general(x, y, (((0,), (0,)), ((), ())), preferred_element_type=f32)

    load_g(0).start()
    load_a_part(0).start()
    load_g(1).start()
    load_a_part(1).start()
    load_g(2).start()

    barrier = pltpu.get_barrier_semaphore()
    for way in (RIGHT, LEFT):
        pl.semaphore_signal(barrier, inc=1, device_id={"dp": to[way]}, device_id_type=MESH)

    for part, kind in ((0, FAR0), (1, FAR1)):
        at = pl.ds(0, CUT) if part == 0 else pl.ds(CUT, rows - CUT)
        load_a_part(part).wait()
        for way in (RIGHT, LEFT):
            if part == 0:
                load_g(way).wait()
            snd[0, 0, way, at] = dot(abuf[0, :, at], gbuf[way]).astype(snd.dtype)
            if part == 0 and way == RIGHT:
                pl.semaphore_wait(barrier, 2)
            copy(0, kind, way).start()
    for u in (3, 4, 5):
        load_g(u).start()
    load_a(1).start()

    @pl.loop(2, units)
    def unit(u):
        m, j = u // per, lax.rem(u, per)

        @pl.when((u > 2) & (u + 3 < units))
        def _():
            load_g(u + 3).start()

        @pl.when(j == 0)
        def _():
            load_a(m).wait()

            @pl.when(m + 1 < matrices)
            def _():
                load_a(m + 1).start()

        load_g(u).wait()
        side = lax.rem(m, 2)
        slot = pick(j, [0, 0, 0, 0, 1, 2, 3 + 2 * side, 4 + 2 * side])
        term[slot] = dot(abuf[side], gbuf[lax.rem(u, G_SLOTS)])

        for way in (RIGHT, LEFT):

            @pl.when(j == way)
            def _():
                snd[m, 0, way] = term[0].astype(snd.dtype)
                copy(m, FAR0, way).start()
                copy(m, FAR1, way).start()

            @pl.when(j == 2 + way)
            def _():
                snd[m, 1, way] = term[0].astype(snd.dtype)
                copy(m, RAW, way).start()

        @pl.when(j == per - 1)
        def _():
            add_far(m)

            @pl.when(m >= 1)
            def _():
                finish(m - 1)

            @pl.when(m >= 2)
            def _():
                pass_on(m - 2)

    finish(matrices - 1)
    pass_on(matrices - 2)
    pass_on(matrices - 1)

    @pl.loop(0, matrices)
    def _(m):
        for way in (RIGHT, LEFT):
            for kind in (SECOND, ON):
                copy(m, kind, way).wait_recv()
            for kind in range(KINDS):
                copy(m, kind, way).wait_send()


def write(held, out, sem):
    pieces = []
    for m in range(held.shape[0]):
        for r in range(0, held.shape[1], held.shape[1] // 2):
            at = (m, pl.ds(r, held.shape[1] // 2))
            pieces.append(pltpu.make_async_copy(held.at[at], out.at[at], sem.at[len(pieces)]))
    for piece in pieces:
        piece.start()
    for piece in pieces:
        piece.wait()


def solution(mesh):
    n = mesh.shape["dp"]

    def local(a, g):
        matrices, tokens, rows = a.shape[1:]
        wide = g.shape[3]
        half = wide // n // 2
        bf16, f32 = jnp.bfloat16, jnp.float32
        held = pl.pallas_call(
            functools.partial(kernel, n),
            out_shape=pltpu.VMEM((matrices, rows, wide), bf16),
            in_specs=[pl.BlockSpec(memory_space=pl.ANY)] * 2,
            out_specs=pl.BlockSpec(memory_space=pltpu.VMEM),
            scratch_shapes=[
                pltpu.VMEM((2, tokens, rows), bf16),
                pltpu.VMEM((G_SLOTS, tokens, half), bf16),
                pltpu.VMEM((7, rows, half), f32),
                pltpu.VMEM((matrices, 3, 2, rows, half), bf16),
                pltpu.VMEM((matrices, 3, 2, rows, half), bf16),
                pltpu.SemaphoreType.DMA((3,)),
                pltpu.SemaphoreType.DMA((G_SLOTS,)),
                pltpu.SemaphoreType.DMA((matrices, KINDS, 2)),
                pltpu.SemaphoreType.DMA((matrices, KINDS, 2)),
            ],
            compiler_params=pltpu.CompilerParams(
                collective_id=0, has_side_effects=True, vmem_limit_bytes=VMEM_LIMIT
            ),
        )(a, g)
        return pl.pallas_call(
            write,
            out_shape=jax.ShapeDtypeStruct(held.shape, bf16),
            in_specs=[pl.BlockSpec(memory_space=pltpu.VMEM)],
            out_specs=pl.BlockSpec(memory_space=pl.ANY),
            scratch_shapes=[pltpu.SemaphoreType.DMA((2 * matrices,))],
            compiler_params=pltpu.CompilerParams(vmem_limit_bytes=2 * 1024 * 1024),
        )(pltpu.with_memory_space_constraint(held, pltpu.VMEM))

    return jax.shard_map(
        local,
        mesh=mesh,
        in_specs=(P(("rep", "dp")), P(("rep", "dp"))),
        out_specs=P("rep"),
        check_vma=False,
    )
```

```python
import functools

import jax
import jax.numpy as jnp
from jax import lax
from jax.experimental import pallas as pl
from jax.experimental.pallas import tpu as pltpu
from jax.sharding import PartitionSpec as P

MESH = pl.DeviceIdType.MESH
RIGHT, LEFT = 0, 1
FAR, RAW, SUM, WHOLE, ON = range(5)
CUT = ON
G_SLOTS = 4
A_UNIT = 3
STRIP = 128
CUTS = (1, 1, 1, 2, 2, 3)
VMEM_LIMIT = 53000000


def kernel(n, a, g, out, abuf, gbuf, term, snd, rcv, a_sem, g_sem, c_sem, send_sem, far_sem, near_sem, whole_sem, on_sem):
    matrices, tokens, rows = a.shape[1:]
    half = g.shape[3] // n // 2
    quarter = half // 2
    per = 2 * n
    units = matrices * per
    f32 = jnp.float32
    me = lax.axis_index("dp")
    to = [lax.rem(me + 1, n), lax.rem(me + n - 1, n)]

    def columns(owner, first, width):
        return pl.ds(pl.multiple_of(owner * (2 * half) + first, width), width)

    def block(owner, b):
        return columns(owner, b * quarter, quarter)

    def load_a(m):
        return pltpu.make_async_copy(a.at[0, m], abuf.at[lax.rem(m, 2)], a_sem.at[lax.rem(m, 2)])

    def pick(j, values):
        out = values[-1]
        for i, value in reversed(list(enumerate(values[:-1]))):
            out = jnp.where(j == i, value, out)
        return out

    order = [(2, 1), (2, 0), (1, 0), (n - 1, 1), (1, 1), (n - 1, 0), (0, 0), (0, 1)]

    def load_g(u):
        m, j = u // per, lax.rem(u, per)
        owner = lax.rem(me + pick(j, [o for o, _ in order]), n)
        slot, h = lax.rem(u, G_SLOTS), pick(j, [h for _, h in order])
        return [
            pltpu.make_async_copy(
                g.at[0, m, :, block(owner, 2 * b + h)], gbuf.at[slot, :, pl.ds(b * quarter, quarter)], g_sem.at[slot]
            )
            for b in (0, 1)
        ]

    def wait_g(u):
        slot = lax.rem(u, G_SLOTS)
        pltpu.make_async_copy(g.at[0, 0, :, pl.ds(0, half)], gbuf.at[slot], g_sem.at[slot]).wait()

    def start_g(u):
        for load in load_g(u):
            load.start()

    def copy(m, kind, way, at=()):
        if kind == WHOLE:
            src = dst = out.at[m, :, columns(me, 0, 2 * half)]
        elif kind == ON:
            src = dst = out.at[m, :, columns(to[1 - way], way * half, half)]
        else:
            step = FAR if kind > CUT else kind
            src, dst = snd.at[(m, step, way, *at)], rcv.at[(m, step, way, *at)]
        if kind == WHOLE:
            sem = whole_sem.at[m, way]
        elif kind == ON:
            sem = on_sem
        else:
            sem = near_sem.at[m] if kind in (RAW, SUM) else far_sem.at[m, way]
        return remote(src, dst, sem, way)

    def remote(src, dst, sem, way):
        return pltpu.make_async_remote_copy(
            src_ref=src,
            dst_ref=dst,
            send_sem=send_sem.at[way],
            recv_sem=sem,
            device_id={"dp": to[way]},
            device_id_type=MESH,
        )

    def wait_near(m):
        both = rcv.at[m, pl.ds(RAW, 2)]
        remote(both, both, near_sem.at[m], RIGHT).wait_recv()

    def wait_on():
        where = out.at[:, :, pl.ds(0, 2 * half)]
        remote(where, where, on_sem, RIGHT).wait_recv()

    def wait_sent(way):
        where = out.at[:, :, pl.ds(0, (n - 1) * 2 * half)]
        remote(where, where, on_sem, way).wait_send()

    def add_far(m, way):
        copy(m, FAR, way).wait_recv()
        total = term[1 + way] + rcv[m, FAR, way].astype(f32)
        snd[m, SUM, way] = total.astype(snd.dtype)
        copy(m, SUM, way).start()

    def finish(m):
        wait_near(m)
        for h in (0, 1):
            total = term[3 + 2 * lax.rem(m, 2) + h] + rcv[m, RAW, h].astype(f32)
            total = total + rcv[m, SUM, 1 - h].astype(f32)
            for b in (0, 1):
                out[m, :, block(me, 2 * b + h)] = total[:, b * quarter : (b + 1) * quarter].astype(out.dtype)
        for way in (RIGHT, LEFT):
            copy(m, WHOLE, way).start()

    def pass_on(m):
        for way in (RIGHT, LEFT):
            copy(m, WHOLE, way).wait_recv()
            copy(m, ON, way).start()

    def dot(x, y):
        return lax.dot_general(x, y, (((0,), (0,)), ((), ())), preferred_element_type=f32)

    strips = rows // STRIP
    cuts, last = [], 0
    for i, count in enumerate(CUTS):
        at = pl.ds(last % strips * STRIP, count * STRIP), pl.ds(last // strips * quarter, quarter)
        last += count
        cuts.append((CUT + 1 + i, last - 1, at))
    far = lax.rem(me + 2, n)

    def strip(r):
        return pl.ds(pl.multiple_of(r * STRIP, STRIP), STRIP)

    def load_strip(r):
        return pltpu.make_async_copy(a.at[0, 0, :, strip(r)], abuf.at[0, :, strip(r)], c_sem.at[r])

    def load_far(b):
        return pltpu.make_async_copy(g.at[0, 0, :, columns(far, b * half, half)], gbuf.at[b], c_sem.at[strips + b])

    load_strip(0).start()
    load_far(0).start()

    barrier = pltpu.get_barrier_semaphore()
    for way in (RIGHT, LEFT):
        pl.semaphore_signal(barrier, inc=1, device_id={"dp": to[way]}, device_id_type=MESH)

    for r in range(1, strips):
        load_strip(r).start()
    load_far(1).start()
    start_g(2)

    @pl.loop(0, 2 * strips)
    def _(i):
        idle = i < 0
        b = jnp.where(i < strips, 0, 1)
        r = jnp.where(idle, 0, i - b * strips)

        @pl.when((i >= 0) & (b == 0))
        def _():
            load_strip(r).wait()

        @pl.when((i == 0) | (i == strips))
        def _():
            load_far(b).wait()

        @pl.when(i == 0)
        def _():
            start_g(3)

        @pl.when(i == strips)
        def _():
            start_g(4)

        value = dot(abuf[jnp.where(idle, 1, 0), :, strip(r)], gbuf[jnp.where(idle, 3, b)])
        to_column = pl.ds(pl.multiple_of(b * quarter, quarter), quarter)
        for way, side in ((RIGHT, 1), (LEFT, 0)):
            snd[0, FAR, way, strip(r), to_column] = value[:, side * quarter : (side + 1) * quarter].astype(snd.dtype)

        @pl.when(i == 0)
        def _():
            pl.semaphore_wait(barrier, 2)

        for kind, end, at in cuts:

            @pl.when(i == end)
            def _():
                for way in (RIGHT, LEFT):
                    copy(0, kind, way, at).start()

    @pl.loop(2, units)
    def unit(u):
        m, j = u // per, lax.rem(u, per)

        @pl.when((u > 2) & (u + 3 < units))
        def _():
            start_g(u + 3)

        @pl.when(u == 3)
        def _():
            start_g(5)

        @pl.when(j == 0)
        def _():
            load_a(m).wait()

        @pl.when((j == A_UNIT) & (m + 1 < matrices))
        def _():
            load_a(m + 1).start()

        wait_g(u)
        side = lax.rem(m, 2)
        slot = pick(j, [0, 0, 0, 0, 1, 2, 3 + 2 * side, 4 + 2 * side])
        term[slot] = dot(abuf[side], gbuf[lax.rem(u, G_SLOTS)])

        for way in (RIGHT, LEFT):

            @pl.when(j == way)
            def _():
                snd[m, 0, way] = term[0].astype(snd.dtype)
                copy(m, FAR, way).start()

            @pl.when(j == 2 + way)
            def _():
                snd[m, 1, way] = term[0].astype(snd.dtype)
                copy(m, RAW, way).start()

            @pl.when(j == 4 + way)
            def _():
                add_far(m, way)

        @pl.when(j == per - 1)
        def _():
            @pl.when(m >= 1)
            def _():
                finish(m - 1)

            @pl.when(m >= 2)
            def _():
                pass_on(m - 2)

    finish(matrices - 1)
    pass_on(matrices - 2)
    pass_on(matrices - 1)

    wait_on()
    for way in (RIGHT, LEFT):
        wait_sent(way)


def write(held, out, sem):
    pieces = []
    for m in range(held.shape[0]):
        for r in range(0, held.shape[1], held.shape[1] // 2):
            at = (m, pl.ds(r, held.shape[1] // 2))
            pieces.append(pltpu.make_async_copy(held.at[at], out.at[at], sem.at[len(pieces)]))
    for piece in pieces:
        piece.start()
    for piece in pieces:
        piece.wait()


def solution(mesh):
    n = mesh.shape["dp"]

    def local(a, g):
        matrices, tokens, rows = a.shape[1:]
        wide = g.shape[3]
        half = wide // n // 2
        bf16, f32 = jnp.bfloat16, jnp.float32
        held = pl.pallas_call(
            functools.partial(kernel, n),
            out_shape=pltpu.VMEM((matrices, rows, wide), bf16),
            in_specs=[pl.BlockSpec(memory_space=pl.ANY)] * 2,
            out_specs=pl.BlockSpec(memory_space=pltpu.VMEM),
            scratch_shapes=[
                pltpu.VMEM((2, tokens, rows), bf16),
                pltpu.VMEM((G_SLOTS, tokens, half), bf16),
                pltpu.VMEM((7, rows, half), f32),
                pltpu.VMEM((matrices, 3, 2, rows, half), bf16),
                pltpu.VMEM((matrices, 3, 2, rows, half), bf16),
                pltpu.SemaphoreType.DMA((2,)),
                pltpu.SemaphoreType.DMA((G_SLOTS,)),
                pltpu.SemaphoreType.DMA((rows // STRIP + 2,)),
                pltpu.SemaphoreType.DMA((2,)),
                pltpu.SemaphoreType.DMA((matrices, 2)),
                pltpu.SemaphoreType.DMA((matrices,)),
                pltpu.SemaphoreType.DMA((matrices, 2)),
                pltpu.SemaphoreType.DMA,
            ],
            compiler_params=pltpu.CompilerParams(
                collective_id=0, has_side_effects=True, vmem_limit_bytes=VMEM_LIMIT
            ),
        )(a, g)
        return pl.pallas_call(
            write,
            out_shape=jax.ShapeDtypeStruct(held.shape, bf16),
            in_specs=[pl.BlockSpec(memory_space=pltpu.VMEM)],
            out_specs=pl.BlockSpec(memory_space=pl.ANY),
            scratch_shapes=[pltpu.SemaphoreType.DMA((2 * matrices,))],
            compiler_params=pltpu.CompilerParams(vmem_limit_bytes=2 * 1024 * 1024),
        )(pltpu.with_memory_space_constraint(held, pltpu.VMEM))

    return jax.shard_map(
        local,
        mesh=mesh,
        in_specs=(P(("rep", "dp")), P(("rep", "dp"))),
        out_specs=P("rep"),
        check_vma=False,
    )
```

```python
import functools

import jax
import jax.numpy as jnp
from jax import lax
from jax.experimental import pallas as pl
from jax.experimental.pallas import tpu as pltpu
from jax.sharding import PartitionSpec as P

MESH = pl.DeviceIdType.MESH
RIGHT, LEFT = 0, 1
FAR, RAW, SUM, WHOLE, ON = range(5)
G_SLOTS = 4
A_UNIT = 3
CHUNKS = 2
STRIP = 128
CUTS = (1, 1, 1, 2, 2, 3)
VMEM_LIMIT = 53000000


def kernel(n, a, g, out, abuf, gbuf, term, snd, rcv, a_sem, g_sem, c_sem, send_sem, far_sem, near_sem, whole_sem, on_sem):
    matrices, tokens, rows = a.shape[1:]
    half = g.shape[3] // n // 2
    quarter = half // 2
    per = 2 * n
    units = matrices * per
    f32 = jnp.float32
    me = lax.axis_index("dp")
    to = [lax.rem(me + 1, n), lax.rem(me + n - 1, n)]

    def columns(owner, first, width):
        return pl.ds(pl.multiple_of(owner * (2 * half) + first, width), width)

    def block(owner, b):
        return columns(owner, b * quarter, quarter)

    def load_a(m):
        return pltpu.make_async_copy(a.at[0, m], abuf.at[lax.rem(m, 2)], a_sem.at[lax.rem(m, 2)])

    def pick(j, values):
        out = values[-1]
        for i, value in reversed(list(enumerate(values[:-1]))):
            out = jnp.where(j == i, value, out)
        return out

    order = [(2, 1), (2, 0), (1, 0), (n - 1, 1), (1, 1), (n - 1, 0), (0, 0), (0, 1)]

    def load_g(u):
        m, j = u // per, lax.rem(u, per)
        owner = lax.rem(me + pick(j, [o for o, _ in order]), n)
        slot, h = lax.rem(u, G_SLOTS), pick(j, [h for _, h in order])
        return [
            pltpu.make_async_copy(
                g.at[0, m, :, block(owner, 2 * b + h)], gbuf.at[slot, :, pl.ds(b * quarter, quarter)], g_sem.at[slot]
            )
            for b in (0, 1)
        ]

    def wait_g(u):
        slot = lax.rem(u, G_SLOTS)
        pltpu.make_async_copy(g.at[0, 0, :, pl.ds(0, half)], gbuf.at[slot], g_sem.at[slot]).wait()

    def start_g(u):
        for load in load_g(u):
            load.start()

    def copy(m, kind, way, at=()):
        if kind == WHOLE:
            src = dst = out.at[m, :, columns(me, 0, 2 * half)]
        elif kind == ON:
            src = dst = out.at[m, :, columns(to[1 - way], way * half, half)]
        else:
            src, dst = snd.at[(m, kind, way, *at)], rcv.at[(m, kind, way, *at)]
        if kind == WHOLE:
            sem = whole_sem.at[m, way]
        elif kind == ON:
            sem = on_sem
        else:
            sem = near_sem.at[m] if kind in (RAW, SUM) else far_sem.at[m, way]
        return remote(src, dst, sem, way)

    def remote(src, dst, sem, way):
        return pltpu.make_async_remote_copy(
            src_ref=src,
            dst_ref=dst,
            send_sem=send_sem.at[way],
            recv_sem=sem,
            device_id={"dp": to[way]},
            device_id_type=MESH,
        )

    def wait_near(m):
        both = rcv.at[m, pl.ds(RAW, 2)]
        remote(both, both, near_sem.at[m], RIGHT).wait_recv()

    def wait_on():
        where = out.at[:, :, pl.ds(0, 2 * half)]
        remote(where, where, on_sem, RIGHT).wait_recv()

    def wait_sent(way):
        where = out.at[:, :, pl.ds(0, (n - 1) * 2 * half)]
        remote(where, where, on_sem, way).wait_send()

    def add_far(m, way):
        copy(m, FAR, way).wait_recv()
        total = term[1 + way] + rcv[m, FAR, way].astype(f32)
        snd[m, SUM, way] = total.astype(snd.dtype)
        copy(m, SUM, way).start()

    def finish(m):
        wait_near(m)
        for h in (0, 1):
            total = term[3 + 2 * lax.rem(m, 2) + h] + rcv[m, RAW, h].astype(f32)
            total = total + rcv[m, SUM, 1 - h].astype(f32)
            for b in (0, 1):
                out[m, :, block(me, 2 * b + h)] = total[:, b * quarter : (b + 1) * quarter].astype(out.dtype)
        for way in (RIGHT, LEFT):
            copy(m, WHOLE, way).start()

    def pass_on(m):
        for way in (RIGHT, LEFT):
            copy(m, WHOLE, way).wait_recv()
            copy(m, ON, way).start()

    def dot(x, y):
        return lax.dot_general(x, y, (((0,), (0,)), ((), ())), preferred_element_type=f32)

    strips = rows // STRIP
    cuts, last = [], 0
    for count in CUTS:
        at = pl.ds(last % strips * STRIP, count * STRIP), pl.ds(last // strips * quarter, quarter)
        last += count
        cuts.append((last - 1, at))
    far = lax.rem(me + 2, n)

    def strip(r):
        return pl.ds(pl.multiple_of(r * STRIP, STRIP), STRIP)

    def load_strip(r):
        return pltpu.make_async_copy(a.at[0, 0, :, strip(r)], abuf.at[0, :, strip(r)], c_sem.at[2 * CHUNKS - 1 + r])

    def load_far(b):
        return pltpu.make_async_copy(g.at[0, 0, :, columns(far, b * half, half)], gbuf.at[b], g_sem.at[b])

    chunks = [pl.ds(c * (tokens // CHUNKS), tokens // CHUNKS) for c in range(CHUNKS)]

    def load_first(c):
        at, cut = chunks[c], pl.ds(0, STRIP)
        return [
            pltpu.make_async_copy(a.at[0, 0, at, cut], abuf.at[0, at, cut], c_sem.at[c]),
            pltpu.make_async_copy(g.at[0, 0, at, columns(far, 0, half)], gbuf.at[0, at], c_sem.at[CHUNKS + c]),
        ]

    for c in range(CHUNKS):
        for load in load_first(c):
            load.start()

    barrier = pltpu.get_barrier_semaphore()
    for way in (RIGHT, LEFT):
        pl.semaphore_signal(barrier, inc=1, device_id={"dp": to[way]}, device_id_type=MESH)

    for r in range(1, strips):
        load_strip(r).start()
    load_far(1).start()
    start_g(2)

    def keep_far(b, r, value):
        to_column = pl.ds(pl.multiple_of(b * quarter, quarter), quarter)
        for way, side in ((RIGHT, 1), (LEFT, 0)):
            piece = value[:, side * quarter : (side + 1) * quarter]
            snd[0, FAR, way, strip(r), to_column] = piece.astype(snd.dtype)

    def send_far(at):
        for way in (RIGHT, LEFT):
            copy(0, FAR, way, at).start()

    value = None
    for c in range(CHUNKS):
        for load in load_first(c):
            load.wait()
        product = dot(abuf[0, chunks[c], pl.ds(0, STRIP)], gbuf[0, chunks[c]])
        value = product if value is None else value + product
    keep_far(0, 0, value)
    pl.semaphore_wait(barrier, 2)
    send_far(cuts[0][1])
    start_g(3)

    @pl.loop(1, 2 * strips)
    def _(i):
        b = i // strips
        r = lax.rem(i, strips)

        @pl.when(b == 0)
        def _():
            load_strip(r).wait()

        @pl.when(i == strips)
        def _():
            load_far(1).wait()
            start_g(4)

        keep_far(b, r, dot(abuf[0, :, strip(r)], gbuf[b]))

        for end, at in cuts[1:]:

            @pl.when(i == end)
            def _():
                send_far(at)

    @pl.loop(2, units)
    def unit(u):
        m, j = u // per, lax.rem(u, per)

        @pl.when((u > 2) & (u + 3 < units))
        def _():
            start_g(u + 3)

        @pl.when(u == 3)
        def _():
            start_g(5)

        @pl.when(j == 0)
        def _():
            load_a(m).wait()

        @pl.when((j == A_UNIT) & (m + 1 < matrices))
        def _():
            load_a(m + 1).start()

        wait_g(u)
        side = lax.rem(m, 2)
        slot = pick(j, [0, 0, 0, 0, 1, 2, 3 + 2 * side, 4 + 2 * side])
        term[slot] = dot(abuf[side], gbuf[lax.rem(u, G_SLOTS)])

        for way in (RIGHT, LEFT):

            @pl.when(j == way)
            def _():
                snd[m, 0, way] = term[0].astype(snd.dtype)
                copy(m, FAR, way).start()

            @pl.when(j == 2 + way)
            def _():
                snd[m, 1, way] = term[0].astype(snd.dtype)
                copy(m, RAW, way).start()

            @pl.when(j == 4 + way)
            def _():
                add_far(m, way)

        @pl.when(j == per - 1)
        def _():
            @pl.when(m >= 1)
            def _():
                finish(m - 1)

            @pl.when(m >= 2)
            def _():
                pass_on(m - 2)

    finish(matrices - 1)
    pass_on(matrices - 2)
    pass_on(matrices - 1)

    wait_on()
    for way in (RIGHT, LEFT):
        wait_sent(way)


def write(held, out, sem):
    pieces = [held.shape[1] // 2 * i for i in (0, 1)]
    for m in range(held.shape[0]):
        for r in pieces:
            at = (m, pl.ds(r, held.shape[1] // 2))
            pltpu.make_async_copy(held.at[at], out.at[at], sem).start()
    pltpu.make_async_copy(held, out, sem).wait()


def solution(mesh):
    n = mesh.shape["dp"]

    def local(a, g):
        matrices, tokens, rows = a.shape[1:]
        wide = g.shape[3]
        half = wide // n // 2
        bf16, f32 = jnp.bfloat16, jnp.float32
        held = pl.pallas_call(
            functools.partial(kernel, n),
            out_shape=pltpu.VMEM((matrices, rows, wide), bf16),
            in_specs=[pl.BlockSpec(memory_space=pl.ANY)] * 2,
            out_specs=pl.BlockSpec(memory_space=pltpu.VMEM),
            scratch_shapes=[
                pltpu.VMEM((2, tokens, rows), bf16),
                pltpu.VMEM((G_SLOTS, tokens, half), bf16),
                pltpu.VMEM((7, rows, half), f32),
                pltpu.VMEM((matrices, 3, 2, rows, half), bf16),
                pltpu.VMEM((matrices, 3, 2, rows, half), bf16),
                pltpu.SemaphoreType.DMA((2,)),
                pltpu.SemaphoreType.DMA((G_SLOTS,)),
                pltpu.SemaphoreType.DMA((2 * CHUNKS + rows // STRIP - 1,)),
                pltpu.SemaphoreType.DMA((2,)),
                pltpu.SemaphoreType.DMA((matrices, 2)),
                pltpu.SemaphoreType.DMA((matrices,)),
                pltpu.SemaphoreType.DMA((matrices, 2)),
                pltpu.SemaphoreType.DMA,
            ],
            compiler_params=pltpu.CompilerParams(
                collective_id=0, has_side_effects=True, vmem_limit_bytes=VMEM_LIMIT
            ),
        )(a, g)
        return pl.pallas_call(
            write,
            out_shape=jax.ShapeDtypeStruct(held.shape, bf16),
            in_specs=[pl.BlockSpec(memory_space=pltpu.VMEM)],
            out_specs=pl.BlockSpec(memory_space=pl.ANY),
            scratch_shapes=[pltpu.SemaphoreType.DMA],
            compiler_params=pltpu.CompilerParams(vmem_limit_bytes=2 * 1024 * 1024),
        )(pltpu.with_memory_space_constraint(held, pltpu.VMEM))

    return jax.shard_map(
        local,
        mesh=mesh,
        in_specs=(P(("rep", "dp")), P(("rep", "dp"))),
        out_specs=P("rep"),
        check_vma=False,
    )
```

```python
import functools

import jax
import jax.numpy as jnp
from jax import lax
from jax.experimental import pallas as pl
from jax.experimental.pallas import tpu as pltpu
from jax.sharding import PartitionSpec as P

MESH = pl.DeviceIdType.MESH
RIGHT, LEFT = 0, 1
FAR, RAW, SUM, WHOLE, ON = range(5)
G_SLOTS = 4
A_UNIT = 3
CHUNKS = 2
STRIP = 128
CUTS = (1, 1, 1, 1, 1, 1, 2, 2)
VMEM_LIMIT = 53000000


def kernel(n, a, g, out, abuf, gbuf, term, snd, rcv, a_sem, g_sem, c_sem, send_sem, far_sem, near_sem, whole_sem, on_sem):
    matrices, tokens, rows = a.shape[1:]
    half = g.shape[3] // n // 2
    quarter = half // 2
    per = 2 * n
    units = matrices * per
    f32 = jnp.float32
    me = lax.axis_index("dp")
    to = [lax.rem(me + 1, n), lax.rem(me + n - 1, n)]

    def columns(owner, first, width):
        return pl.ds(pl.multiple_of(owner * (2 * half) + first, width), width)

    def block(owner, b):
        return columns(owner, b * quarter, quarter)

    def load_a(m):
        return pltpu.make_async_copy(a.at[0, m], abuf.at[lax.rem(m, 2)], a_sem.at[lax.rem(m, 2)])

    def pick(j, values):
        out = values[-1]
        for i, value in reversed(list(enumerate(values[:-1]))):
            out = jnp.where(j == i, value, out)
        return out

    order = [(2, 1), (2, 0), (1, 0), (n - 1, 1), (1, 1), (n - 1, 0), (0, 0), (0, 1)]

    def load_g(u):
        m, j = u // per, lax.rem(u, per)
        owner = lax.rem(me + pick(j, [o for o, _ in order]), n)
        slot, h = lax.rem(u, G_SLOTS), pick(j, [h for _, h in order])
        return [
            pltpu.make_async_copy(
                g.at[0, m, :, block(owner, 2 * b + h)], gbuf.at[slot, :, pl.ds(b * quarter, quarter)], g_sem.at[slot]
            )
            for b in (0, 1)
        ]

    def wait_g(u):
        slot = lax.rem(u, G_SLOTS)
        pltpu.make_async_copy(g.at[0, 0, :, pl.ds(0, half)], gbuf.at[slot], g_sem.at[slot]).wait()

    def start_g(u):
        for load in load_g(u):
            load.start()

    def copy(m, kind, way, at=()):
        if kind == WHOLE:
            src = dst = out.at[m, :, columns(me, 0, 2 * half)]
        elif kind == ON:
            src = dst = out.at[m, :, columns(to[1 - way], way * half, half)]
        else:
            src, dst = snd.at[(m, kind, way, *at)], rcv.at[(m, kind, way, *at)]
        if kind == WHOLE:
            sem = whole_sem.at[m, way]
        elif kind == ON:
            sem = on_sem
        else:
            sem = near_sem.at[m] if kind in (RAW, SUM) else far_sem.at[m, way]
        return remote(src, dst, sem, way)

    def remote(src, dst, sem, way):
        return pltpu.make_async_remote_copy(
            src_ref=src,
            dst_ref=dst,
            send_sem=send_sem.at[way],
            recv_sem=sem,
            device_id={"dp": to[way]},
            device_id_type=MESH,
        )

    def wait_near(m):
        both = rcv.at[m, pl.ds(RAW, 2)]
        remote(both, both, near_sem.at[m], RIGHT).wait_recv()

    def wait_on():
        where = out.at[:, :, pl.ds(0, 2 * half)]
        remote(where, where, on_sem, RIGHT).wait_recv()

    def wait_sent(way):
        where = out.at[:, :, pl.ds(0, (n - 1) * 2 * half)]
        remote(where, where, on_sem, way).wait_send()

    def add_far(m, way):
        copy(m, FAR, way).wait_recv()
        total = term[1 + way] + rcv[m, FAR, way].astype(f32)
        snd[m, SUM, way] = total.astype(snd.dtype)
        copy(m, SUM, way).start()

    def finish(m):
        wait_near(m)
        for h in (0, 1):
            total = term[3 + 2 * lax.rem(m, 2) + h] + rcv[m, RAW, h].astype(f32)
            total = total + rcv[m, SUM, 1 - h].astype(f32)
            for b in (0, 1):
                out[m, :, block(me, 2 * b + h)] = total[:, b * quarter : (b + 1) * quarter].astype(out.dtype)
        for way in (RIGHT, LEFT):
            copy(m, WHOLE, way).start()

    def pass_on(m):
        for way in (RIGHT, LEFT):
            copy(m, WHOLE, way).wait_recv()
            copy(m, ON, way).start()

    def dot(x, y):
        return lax.dot_general(x, y, (((0,), (0,)), ((), ())), preferred_element_type=f32)

    strips = rows // STRIP
    cuts, last = [], 0
    for count in CUTS:
        at = pl.ds(last % strips * STRIP, count * STRIP), pl.ds(last // strips * quarter, quarter)
        last += count
        cuts.append((last - 1, at))
    far = lax.rem(me + 2, n)

    def strip(r):
        return pl.ds(pl.multiple_of(r * STRIP, STRIP), STRIP)

    def load_strip(r):
        return pltpu.make_async_copy(a.at[0, 0, :, strip(r)], abuf.at[0, :, strip(r)], c_sem.at[2 * CHUNKS - 1 + r])

    def load_far(b):
        return pltpu.make_async_copy(g.at[0, 0, :, columns(far, b * half, half)], gbuf.at[b], g_sem.at[b])

    chunks = [pl.ds(c * (tokens // CHUNKS), tokens // CHUNKS) for c in range(CHUNKS)]

    def load_first(c):
        at, cut = chunks[c], pl.ds(0, STRIP)
        return [
            pltpu.make_async_copy(a.at[0, 0, at, cut], abuf.at[0, at, cut], c_sem.at[c]),
            pltpu.make_async_copy(g.at[0, 0, at, columns(far, 0, half)], gbuf.at[0, at], c_sem.at[CHUNKS + c]),
        ]

    for c in range(CHUNKS):
        for load in load_first(c):
            load.start()

    barrier = pltpu.get_barrier_semaphore()
    for way in (RIGHT, LEFT):
        pl.semaphore_signal(barrier, inc=1, device_id={"dp": to[way]}, device_id_type=MESH)

    for r in range(1, strips):
        load_strip(r).start()
    load_far(1).start()
    start_g(2)

    def keep_far(b, r, value):
        to_column = pl.ds(pl.multiple_of(b * quarter, quarter), quarter)
        for way, side in ((RIGHT, 1), (LEFT, 0)):
            piece = value[:, side * quarter : (side + 1) * quarter]
            snd[0, FAR, way, strip(r), to_column] = piece.astype(snd.dtype)

    def send_far(at):
        for way in (RIGHT, LEFT):
            copy(0, FAR, way, at).start()

    value = None
    for c in range(CHUNKS):
        for load in load_first(c):
            load.wait()
        product = dot(abuf[0, chunks[c], pl.ds(0, STRIP)], gbuf[0, chunks[c]])
        value = product if value is None else value + product
    keep_far(0, 0, value)
    pl.semaphore_wait(barrier, 2)
    send_far(cuts[0][1])
    start_g(3)

    @pl.loop(1, 2 * strips)
    def _(i):
        b = i // strips
        r = lax.rem(i, strips)

        @pl.when(b == 0)
        def _():
            load_strip(r).wait()

        @pl.when(i == strips)
        def _():
            load_far(1).wait()
            start_g(4)

        keep_far(b, r, dot(abuf[0, :, strip(r)], gbuf[b]))

        for end, at in cuts[1:]:

            @pl.when(i == end)
            def _():
                send_far(at)

    @pl.loop(2, units)
    def unit(u):
        m, j = u // per, lax.rem(u, per)

        @pl.when((u > 2) & (u + 3 < units))
        def _():
            start_g(u + 3)

        @pl.when(u == 3)
        def _():
            start_g(5)

        @pl.when(j == 0)
        def _():
            load_a(m).wait()

        @pl.when((j == A_UNIT) & (m + 1 < matrices))
        def _():
            load_a(m + 1).start()

        wait_g(u)
        side = lax.rem(m, 2)
        slot = pick(j, [0, 0, 0, 0, 1, 2, 3 + 2 * side, 4 + 2 * side])
        term[slot] = dot(abuf[side], gbuf[lax.rem(u, G_SLOTS)])

        for way in (RIGHT, LEFT):

            @pl.when(j == way)
            def _():
                snd[m, 0, way] = term[0].astype(snd.dtype)
                copy(m, FAR, way).start()

            @pl.when(j == 2 + way)
            def _():
                snd[m, 1, way] = term[0].astype(snd.dtype)
                copy(m, RAW, way).start()

            @pl.when(j == 4 + way)
            def _():
                add_far(m, way)

        @pl.when(j == per - 1)
        def _():
            @pl.when(m >= 1)
            def _():
                finish(m - 1)

            @pl.when(m >= 2)
            def _():
                pass_on(m - 2)

    finish(matrices - 1)
    pass_on(matrices - 2)
    pass_on(matrices - 1)

    wait_on()
    for way in (RIGHT, LEFT):
        wait_sent(way)


def write(held, out, sem):
    pieces = [held.shape[1] // 2 * i for i in (0, 1)]
    for m in range(held.shape[0]):
        for r in pieces:
            at = (m, pl.ds(r, held.shape[1] // 2))
            pltpu.make_async_copy(held.at[at], out.at[at], sem).start()
    pltpu.make_async_copy(held, out, sem).wait()


def solution(mesh):
    n = mesh.shape["dp"]

    def local(a, g):
        matrices, tokens, rows = a.shape[1:]
        wide = g.shape[3]
        half = wide // n // 2
        bf16, f32 = jnp.bfloat16, jnp.float32
        held = pl.pallas_call(
            functools.partial(kernel, n),
            out_shape=pltpu.VMEM((matrices, rows, wide), bf16),
            in_specs=[pl.BlockSpec(memory_space=pl.ANY)] * 2,
            out_specs=pl.BlockSpec(memory_space=pltpu.VMEM),
            scratch_shapes=[
                pltpu.VMEM((2, tokens, rows), bf16),
                pltpu.VMEM((G_SLOTS, tokens, half), bf16),
                pltpu.VMEM((7, rows, half), f32),
                pltpu.VMEM((matrices, 3, 2, rows, half), bf16),
                pltpu.VMEM((matrices, 3, 2, rows, half), bf16),
                pltpu.SemaphoreType.DMA((2,)),
                pltpu.SemaphoreType.DMA((G_SLOTS,)),
                pltpu.SemaphoreType.DMA((2 * CHUNKS + rows // STRIP - 1,)),
                pltpu.SemaphoreType.DMA((2,)),
                pltpu.SemaphoreType.DMA((matrices, 2)),
                pltpu.SemaphoreType.DMA((matrices,)),
                pltpu.SemaphoreType.DMA((matrices, 2)),
                pltpu.SemaphoreType.DMA,
            ],
            compiler_params=pltpu.CompilerParams(
                collective_id=0, has_side_effects=True, vmem_limit_bytes=VMEM_LIMIT
            ),
        )(a, g)
        return pl.pallas_call(
            write,
            out_shape=jax.ShapeDtypeStruct(held.shape, bf16),
            in_specs=[pl.BlockSpec(memory_space=pltpu.VMEM)],
            out_specs=pl.BlockSpec(memory_space=pl.ANY),
            scratch_shapes=[pltpu.SemaphoreType.DMA],
            compiler_params=pltpu.CompilerParams(vmem_limit_bytes=2 * 1024 * 1024),
        )(pltpu.with_memory_space_constraint(held, pltpu.VMEM))

    return jax.shard_map(
        local,
        mesh=mesh,
        in_specs=(P(("rep", "dp")), P(("rep", "dp"))),
        out_specs=P("rep"),
        check_vma=False,
    )
```
